32 devices in a mesh: cuts: 4 (over z), dom: 8 (over y, x, core).
Axes of the slice: x: 2, y: 2, z: 4, core: 2. Of those that a mesh axis runs over, the one named last changes fastest.
Arguments:
- radiation: float32 [256, 8, 512], P('dom', 'cuts'), may hold values from -6 to 6
- electrons: float32 [2, 8, 16384], P(None, 'cuts', 'dom'), may hold values from -6 to 6
- cell_index: int32 [2, 8, 16384], P(None, 'cuts', 'dom'), may hold values from 0 to 254
- cell_offset: float32 [2, 8, 16384], P(None, 'cuts', 'dom'), may hold values from 0 to 1
- kernel_x: float32 [2, 256, 256], replicated, may hold values from -0.25 to 0.25
- kernel_y: float32 [2, 256, 256], replicated, may hold values from -0.25 to 0.25
Outputs:
- radiation_out: float32 [256, 8, 512], P('dom', 'cuts')
- electrons_out: float32 [2, 8, 16384], P(None, 'cuts', 'dom')
The draws below stay inside these ranges and needn't reach their ends.
Inputs may be any that keep to these rules, and one draw needn't show every extreme that they name: `cell_index`: the field is interpolated between cell and cell + 1 in each dimension, so every index stays below 255.
All inputs are finite; a program needn't handle non-finite values.
Results may differ from the reference program's by a relative error of at most 0.0003.
Values sent between devices are 32-bit elements; how exact they have to be, the bound alone decides.
No kernel may reach another device: no remote copies, remote signals or barrier semaphores. Data moves between devices by JAX's collectives and lax.ppermute only.
A program may use at most 64 MiB of HBM per device.

```python
import jax
import jax.numpy as jnp
from jax import lax

G = 256
ITERS = 4
SLICES = 8
ELEC = 16384


def plant(entries, rng, smallest, largest):
    longest = entries.shape.index(max(entries.shape))
    spots = []
    for shift in (0, 1):
        where = [jax.random.randint(jax.random.fold_in(rng, axis), (), 0, length) for axis, length in enumerate(entries.shape)]
        where[longest] = (where[longest] + shift) % entries.shape[longest]
        spots.append(tuple(where))
    return entries.at[spots[0]].set(smallest).at[spots[1]].set(largest)


def shard_levels(rng, dims, pieces, low, largest):
    def one(dim, blocks):
        draws = jax.random.uniform(jax.random.fold_in(jax.random.fold_in(rng, 6), dim), (blocks,), jnp.float32, low / len(pieces), largest / len(pieces))
        return jnp.repeat(jnp.exp(draws), dims[dim] // blocks).reshape((-1,) + (1,) * (len(dims) - dim - 1))

    gain = one(*pieces[0])
    for cut in pieces[1:]:
        gain = gain * one(*cut)
    return gain


def noise(stream_key, shape, scale, limit, shards=(), kind=jnp.bfloat16):
    drawn = jax.random.normal(stream_key, shape, jnp.float32) * scale
    if len(shards) > 0:
        drawn = shard_levels(stream_key, shape, shards, -0.22, 0.18) * drawn
    return jnp.clip(drawn, min=-limit, max=limit).astype(kind)


def setup_inputs(seed: int = 0) -> dict:
    keys = jax.random.split(jax.random.key(seed), 7)
    radiation = noise(keys[0], (G, SLICES, 2 * G), 1.0, 6.0, ((0, 8), (1, 4)), jnp.float32)
    electrons = noise(keys[1], (2, SLICES, ELEC), 1.5, 6.0, ((1, 4), (2, 8)), jnp.float32)
    cell_index = plant(jax.random.randint(keys[2], (2, SLICES, ELEC), 0, G - 1), jax.random.fold_in(keys[2], 1), 0, (G - 1) - 1).astype(jnp.int32)
    cell_offset = jnp.clip(1.0 * jax.random.uniform(keys[3], (2, SLICES, ELEC), jnp.float32) ** shard_levels(keys[3], (2, SLICES, ELEC), ((1, 4), (2, 8)), -0.2, 0.2), 0.0, 1.0)
    kernel_x = noise(keys[4], (2, G, G), (2 * G) ** -0.5, 0.25, (), jnp.float32)
    kernel_y = noise(keys[5], (2, G, G), (2 * G) ** -0.5, 0.25, (), jnp.float32)
    return {"radiation": radiation, "electrons": electrons, "cell_index": cell_index, "cell_offset": cell_offset, "kernel_x": kernel_x, "kernel_y": kernel_y}


coupling = 0.5
phase_step = 1.0
current_gain = 1.0
highest = lax.Precision.HIGHEST


def tent_weights(index, offset):
    grid = jnp.arange(G, dtype=jnp.int32)
    lower = jnp.where(grid[None, :] == index[:, None], 1.0 - offset[:, None], 0.0)
    upper = jnp.where(grid[None, :] == index[:, None] + 1, offset[:, None], 0.0)
    return lower + upper


def one_slice(packed):
    field_s, phase, energy, row_idx, col_idx, row_off, col_off = packed
    weight_x = tent_weights(row_idx, row_off)
    weight_y = tent_weights(col_idx, col_off)
    projected = jnp.dot(weight_x, field_s, precision=highest)
    field_real = jnp.sum(projected[:, :G] * weight_y, axis=1)
    field_imag = jnp.sum(projected[:, G:] * weight_y, axis=1)
    energy = energy - coupling * (field_real * jnp.cos(phase) - field_imag * jnp.sin(phase))
    phase = phase + phase_step * energy
    values = jnp.concatenate([weight_y * jnp.cos(phase)[:, None], -weight_y * jnp.sin(phase)[:, None]], axis=1)
    current = jnp.dot(weight_x.T, values, precision=highest)
    return field_s + current_gain * current, phase, energy


def reference(radiation, electrons, cell_index, cell_offset, kernel_x, kernel_y):
    fields = jnp.transpose(radiation, (1, 0, 2))
    phases = electrons[0]
    energies = electrons[1]
    top = jnp.concatenate([kernel_y[0], kernel_y[1]], axis=1)
    bottom = jnp.concatenate([-kernel_y[1], kernel_y[0]], axis=1)
    big_y = jnp.concatenate([top, bottom], axis=0)
    for number in range(ITERS):
        updated, phases, energies = lax.map(one_slice, (fields, phases, energies, cell_index[0], cell_index[1], cell_offset[0], cell_offset[1]))
        left_re = jnp.einsum("ij,sjc->sic", kernel_x[0], updated, precision=highest)
        left_im = jnp.einsum("ij,sjc->sic", kernel_x[1], updated, precision=highest)
        real_part = left_re[:, :, :G] - left_im[:, :, G:]
        imag_part = left_re[:, :, G:] + left_im[:, :, :G]
        mixed = jnp.concatenate([real_part, imag_part], axis=2)
        mixed = jnp.einsum("sic,cd->sid", mixed, big_y, precision=highest)
        fields = jnp.concatenate([jnp.zeros_like(mixed[:1]), mixed[:-1]], axis=0)
    return jnp.transpose(fields, (1, 0, 2)), jnp.stack([phases, energies])
```

```python
import math

import jax
import jax.numpy as jnp
from jax import lax
from jax.experimental import pallas as pl
from jax.experimental.pallas import tpu as pltpu
from jax.sharding import PartitionSpec as P


ITERS = 4
TILE = 256
BATCH = 8
VMEM_LIMIT = 20 * 2**20

coupling = 0.5
phase_step = 1.0
current_gain = 1.0

f32 = jnp.float32
bf16 = jnp.bfloat16


def split(value):
    high = value.astype(bf16)
    return high, (value - high.astype(f32)).astype(bf16)


def dot(left, right):
    return jnp.dot(left, right, preferred_element_type=f32)


def dot_t(left, right):
    return lax.dot_general(left, right, (((1,), (1,)), ((), ())), preferred_element_type=f32)


def dot3(left, right, product=dot):
    return product(left[0], right[0]) + product(left[1], right[0]) + product(left[0], right[1])


def tent(rows, index, offset):
    distance = lax.broadcasted_iota(jnp.int32, (rows, index.shape[1]), 0).astype(f32) - index
    return jnp.where(distance == 0.0, 1.0 - offset, jnp.where(distance == 1.0, offset, 0.0))


def complex_rows(real, imag):
    rows = real.shape[0] // 2
    return jnp.concatenate([real[:rows] - imag[rows:], real[rows:] + imag[:rows]], axis=0)


def propagate(field, kernel_x, kernel_y):
    half = field.shape[0] // 2
    left = split(kernel_x)
    mixed = split(complex_rows(dot3(left, split(field[:half])), dot3(left, split(field[half:]))))
    return complex_rows(dot3(mixed, split(kernel_y[0])), dot3(mixed, split(kernel_y[1])))


def cell_masks(rows, index):
    shape = (rows, index.shape[1])
    cell = lax.broadcasted_iota(jnp.int32, shape, 0).astype(f32).astype(bf16)
    at = lambda value: jnp.broadcast_to(value.astype(bf16), shape)
    return cell == at(index), cell == at(index + 1.0)


def place(masks, low, high):
    spread = lambda value: jnp.broadcast_to(value, masks[0].shape)
    return jnp.where(masks[0], spread(low), jnp.where(masks[1], spread(high), jnp.zeros(masks[0].shape, low.dtype)))


def place_split(masks, low, high):
    return tuple(place(masks, *pair) for pair in zip(split(low), split(high)))


def gather_tiles(field_ref, cells_ref, high_ref, low_ref, amp_ref):
    half = field_ref.shape[0] // 2
    columns = field_ref.shape[1]
    high, low = split(field_ref[...])
    high_ref[...] = high
    low_ref[...] = low

    def body(t, carry):
        row = lambda n: cells_ref[n, pl.ds(t, 1), :]
        wy = place_split(cell_masks(columns, row(1)), 1.0 - row(3), row(3))
        wx = tent(half, row(0), row(2))
        out = dot3((high_ref[...], low_ref[...]), wy)
        amp_ref[0, pl.ds(t, 1), :] = jnp.sum(out[:half] * wx, axis=0, keepdims=True)
        amp_ref[1, pl.ds(t, 1), :] = jnp.sum(out[half:] * wx, axis=0, keepdims=True)
        return carry

    tiles = cells_ref.shape[1]
    lax.fori_loop(0, tiles, body, 0, unroll=math.gcd(tiles, BATCH))


def first_kernel(where_ref, *refs):
    *blocks, field_ref, amp_ref, state_ref, cells_ref, high_ref, low_ref = refs
    half = field_ref.shape[0] // 2
    count = len(blocks) // 2
    rows = half // len(blocks)
    tiles = cells_ref.shape[1] // count
    for n, ref in enumerate(blocks):
        at = pl.multiple_of(where_ref[n] * rows, rows)
        field_ref[pl.ds(at, rows), :] = ref[:rows, :]
        field_ref[pl.ds(half + at, rows), :] = ref[rows : 2 * rows, :]
        if n < count:
            for k in range(6):
                line = ref[2 * rows + k * tiles : 2 * rows + (k + 1) * tiles, :]
                target = state_ref.at[k] if k < 2 else cells_ref.at[k - 2]
                target[n * tiles : (n + 1) * tiles, :] = line
    gather_tiles(field_ref, cells_ref, high_ref, low_ref, amp_ref)


def gather_kernel(
    fresh_ref, old_ref, own_ref, other_ref, kx_ref, ky_ref, cells_ref, field_ref, amp_ref, high_ref, low_ref
):
    half = field_ref.shape[0] // 2
    total = old_ref[...] + current_gain * (own_ref[...] + other_ref[...])
    moved = propagate(total, kx_ref[...].reshape(2 * half, half), ky_ref)
    field_ref[...] = jnp.where(fresh_ref[0] == 1, 0.0, moved)
    gather_tiles(field_ref, cells_ref, high_ref, low_ref, amp_ref)


def push_kernel(amp_ref, state_ref, cells_ref, current_ref, out_ref, cos_ref, sin_ref):
    half = current_ref.shape[0] // 2
    columns = current_ref.shape[1]
    phase = state_ref[0]
    energy = state_ref[1] - coupling * (amp_ref[0] * jnp.cos(phase) - amp_ref[1] * jnp.sin(phase))
    phase = phase + phase_step * energy
    out_ref[0] = phase
    out_ref[1] = energy
    cos_ref[...] = jnp.cos(phase)
    sin_ref[...] = -jnp.sin(phase)
    current_ref[...] = jnp.zeros_like(current_ref)
    tiles = cells_ref.shape[1]
    batch = math.gcd(tiles, BATCH)

    def weights(t):
        row = lambda n: cells_ref[n, pl.ds(t, 1), :]
        wy = place_split(cell_masks(columns, row(1)), 1.0 - row(3), row(3))
        masks = cell_masks(half, row(0))
        parts = []
        for ref in (cos_ref, sin_ref):
            value = ref[pl.ds(t, 1), :]
            parts.append(place_split(masks, (1.0 - row(2)) * value, row(2) * value))
        return wy, tuple(jnp.concatenate(pair, axis=0) for pair in zip(*parts))

    def body(n, carry):
        built = [weights(n * batch + k) for k in range(batch)]
        join = lambda side, part: jnp.concatenate([item[side][part] for item in built], axis=1)
        wy = join(0, 0), join(0, 1)
        values = join(1, 0), join(1, 1)
        current_ref[...] += dot3(values, wy, dot_t)
        return carry

    lax.fori_loop(0, tiles // batch, body, 0)


def last_kernel(where_ref, old_ref, own_ref, other_ref, kx_ref, ky_ref, rows_ref):
    count, rows = rows_ref.shape[0], rows_ref.shape[1] // 2
    total = old_ref[...] + current_gain * (own_ref[...] + other_ref[...])
    starts = [pl.multiple_of(where_ref[n] * rows, rows) for n in range(count)]
    block = jnp.concatenate([kx_ref[part, pl.ds(at, rows), :] for part in (0, 1) for at in starts], axis=0)
    moved = propagate(total, block, ky_ref)
    for n in range(count):
        rows_ref[n, :rows] = moved[n * rows : (n + 1) * rows]
        rows_ref[n, rows:] = moved[(count + n) * rows : (count + n + 1) * rows]


vmem = pl.BlockSpec(memory_space=pltpu.VMEM)
smem = pl.BlockSpec(memory_space=pltpu.SMEM)


def call(kernel, inputs, outs, scratch, flops):
    shapes = [jax.ShapeDtypeStruct(shape, f32) for shape in outs]
    moved = sum(4 * array.size for array in inputs) + sum(4 * shape.size for shape in shapes)
    return pl.pallas_call(
        kernel,
        out_shape=shapes,
        in_specs=[smem if array.dtype == jnp.int32 else vmem for array in inputs],
        out_specs=[vmem] * len(outs),
        scratch_shapes=scratch,
        compiler_params=pltpu.CompilerParams(vmem_limit_bytes=VMEM_LIMIT),
        cost_estimate=pl.CostEstimate(flops=flops, bytes_accessed=moved, transcendentals=0),
    )(*inputs)


def shards(radiation, electrons, cell_index, cell_offset, kernel_x, kernel_y):
    cuts, dom = lax.axis_size("cuts"), lax.axis_size("dom")
    rows, slices, _ = radiation.shape
    half = kernel_x.shape[1]
    columns = kernel_y.shape[1]
    team = dom // slices
    groups = cuts * slices
    me = lax.axis_index("dom")
    mine = me // team
    cut = lax.axis_index("cuts")

    def seat(cut, number):
        return (1 - cut % 2) * number + (cut % 2) * (slices - 1 - number)

    def number(cut, team_number):
        return cut * slices + seat(cut, team_number)

    group = number(cut, mine)
    tiles = electrons.shape[2] // TILE

    def move(value, target):
        route = []
        for cut in range(cuts):
            for place in range(dom):
                to_cut, to_place = target(cut, place)
                route.append((cut * dom + place, to_cut * dom + to_place))
        return lax.ppermute(value, ("cuts", "dom"), route)

    def pick(array, which):
        return lax.dynamic_index_in_dim(array, which, 0, keepdims=False)

    def to_group(shift, turn=0):
        def target(cut, place):
            home = (number(cut, place // team) + shift) % groups
            return home // slices, seat(home // slices, (home + turn) % slices) * team + place % team

        return target

    def across(value):
        return move(value, lambda cut, place: (cut, place ^ 1))

    parts = jnp.concatenate([electrons, cell_index.astype(f32), cell_offset], axis=0)
    parts = parts.transpose(1, 0, 2).reshape(slices, 6 * tiles, TILE)
    fields = jnp.concatenate([radiation[:, :, :columns], radiation[:, :, columns:]], axis=0).transpose(1, 0, 2)
    payload = jnp.concatenate([fields, parts], axis=1)
    masks = range(0, dom, 2)
    own_blocks = []
    for mask in masks:
        block = pick(payload, seat(cut, (me ^ mask) // team))
        if mask:
            block = move(block, lambda cut, place: (cut, place ^ mask))
        own_blocks.append(block)
    other_blocks = [across(block[: 2 * rows]) for block in own_blocks]
    where = jnp.stack([me ^ mask for mask in masks] + [me ^ 1 ^ mask for mask in masks]).astype(jnp.int32)

    field_shape = (2 * half, columns)
    state_shape = (2, len(masks) * tiles, TILE)
    cells_shape = (4,) + state_shape[1:]
    splits = [pltpu.VMEM(field_shape, bf16)] * 2
    work = 6 * 2 * half * columns * state_shape[1] * TILE
    field, amp, state, cells = call(
        first_kernel,
        [where] + own_blocks + other_blocks,
        [field_shape, state_shape, state_shape, cells_shape],
        splits,
        work,
    )
    cells_of = [cells]
    for step in range(ITERS):
        if step > 0:
            fresh = ((group + step) % groups == 0).astype(jnp.int32).reshape(1)
            field, amp = call(
                gather_kernel,
                [fresh, field, own, other, kernel_x, kernel_y, cells_of[step]],
                [field_shape, state_shape],
                splits,
                work,
            )
        own, state = call(
            push_kernel,
            [amp, state, cells_of[step]],
            [field_shape, state_shape],
            [pltpu.VMEM(state_shape[1:], f32)] * 2,
            work,
        )
        other = across(own)
        if step == 0:
            cells, _ = lax.optimization_barrier((cells, state))
            for later in range(1, ITERS):
                cells_of.append(move(cells, to_group(-later)))
        if step < ITERS - 1:
            state = move(state, to_group(-1))

    def places(home):
        return [seat(home // slices, (home + turn) % slices) * team + me % team for turn in range(slices)]

    field_home = (group + ITERS) % groups
    (blocks,) = call(
        last_kernel,
        [jnp.stack(places(field_home)).astype(jnp.int32), field, own, other, kernel_x, kernel_y],
        [(slices, 2 * rows, columns)],
        [],
        work // 16,
    )
    blocks, state = lax.optimization_barrier((blocks, state))
    landed = []
    for turn in range(slices):
        landed.append(move(blocks[turn], to_group(ITERS, turn)))
    state_home = (group + ITERS - 1) % groups
    seats = places(state_home)
    returned = []
    for turn in range(slices):
        chunk = (seats[turn] ^ seats[0]) // 2
        block = lax.dynamic_slice_in_dim(state, chunk * tiles, tiles, 1)
        returned.append(move(block, to_group(ITERS - 1, turn)))
    order = [(seat(cut, mine) - number) % slices for number in range(slices)]
    landed = jnp.stack(landed)
    landed = [pick(landed, which) for which in order]
    returned = jnp.stack(returned)
    returned = [pick(returned, which).reshape(2, tiles * TILE) for which in order]
    landed[0] = jnp.where(cut == 0, 0.0, landed[0])
    radiation_out = jnp.stack([jnp.concatenate([block[:rows], block[rows:]], axis=1) for block in landed], axis=1)
    return radiation_out, jnp.stack(returned, axis=1)


def solution(mesh):
    placed = (
        P("dom", "cuts", None),
        P(None, "cuts", "dom"),
        P(None, "cuts", "dom"),
        P(None, "cuts", "dom"),
        P(),
        P(),
    )

    return jax.shard_map(
        shards,
        mesh=mesh,
        in_specs=placed,
        out_specs=(P("dom", "cuts", None), P(None, "cuts", "dom")),
        check_vma=False,
    )
```

```python
import math

import jax
import jax.numpy as jnp
from jax import lax
from jax.experimental import pallas as pl
from jax.experimental.pallas import tpu as pltpu
from jax.sharding import PartitionSpec as P


ITERS = 4
TILE = 256
BATCH = 16
CHOICES = 64
REST = 1e-4
VMEM_LIMIT = 16 * 2**20

coupling = 0.5
phase_step = 1.0
current_gain = 1.0

f32 = jnp.float32
bf16 = jnp.bfloat16


def split(value):
    high = value.astype(bf16)
    return high, (value - high.astype(f32)).astype(bf16)


def dot(left, right):
    return jnp.dot(left, right, preferred_element_type=f32)


def dot_t(left, right):
    return lax.dot_general(left, right, (((1,), (1,)), ((), ())), preferred_element_type=f32)


def dot3(left, right, product=dot):
    return product(left[0], right[0]) + product(left[1], right[0]) + product(left[0], right[1])


def dot2(left, right, product=dot):
    return product(left[0], right) + product(left[1], right)


def tent(rows, index, low, high):
    distance = lax.broadcasted_iota(jnp.int32, (rows, index.shape[1]), 0).astype(f32) - index
    return jnp.where(distance == 0.0, low, jnp.where(distance == 1.0, high, 0.0))


def weight_pair(offset):
    small = jnp.minimum(offset, 1.0 - offset)
    ratio = small / jnp.maximum(offset, 1.0 - offset)
    best = jnp.full_like(offset, 2.0)
    large = jnp.ones_like(offset)
    for n in range(CHOICES):
        choice = 1.0 + n / CHOICES
        other = choice * ratio
        miss = jnp.abs(other.astype(bf16).astype(f32) - other) * (1.0 / choice)
        large = jnp.where(miss < best, choice, large)
        best = jnp.minimum(miss, best)
    little = (large * ratio).astype(bf16).astype(f32)
    swap = offset > 0.5
    return jnp.where(swap, little, large), jnp.where(swap, large, little)


def scale_and_rest(cells_ref, rest_ref):
    offset, low, high = cells_ref[3], cells_ref[4], cells_ref[5]
    scale = ((1.0 - offset) * low + offset * high) / (low * low + high * high)
    rest_low = (1.0 - offset) - scale * low
    rest_high = offset - scale * high
    rest_ref[0] = rest_low / scale
    rest_ref[1] = rest_high / scale
    miss = jnp.sum(rest_low * rest_low + rest_high * rest_high)
    return scale, miss > (REST * REST) * 0.5 * offset.size


def complex_rows(real, imag):
    rows = real.shape[0] // 2
    return jnp.concatenate([real[:rows] - imag[rows:], real[rows:] + imag[:rows]], axis=0)


def propagate(field, kernel_x, kernel_y):
    half = field.shape[0] // 2
    left = split(kernel_x)
    mixed = split(complex_rows(dot3(left, split(field[:half])), dot3(left, split(field[half:]))))
    return complex_rows(dot3(mixed, split(kernel_y[0])), dot3(mixed, split(kernel_y[1])))


def cell_masks(rows, index):
    shape = (rows, index.shape[1])
    cell = lax.broadcasted_iota(jnp.int32, shape, 0).astype(f32).astype(bf16)
    at = lambda value: jnp.broadcast_to(value.astype(bf16), shape)
    return cell == at(index), cell == at(index + 1.0)


def place(masks, low, high):
    spread = lambda value: jnp.broadcast_to(value, masks[0].shape)
    return jnp.where(masks[0], spread(low), jnp.where(masks[1], spread(high), jnp.zeros(masks[0].shape, low.dtype)))


def gather_tiles(field_ref, cells_ref, high_ref, low_ref, wx_ref, rest_ref, amp_ref):
    half = field_ref.shape[0] // 2
    columns = field_ref.shape[1]
    tiles = cells_ref.shape[1]
    high, low = split(field_ref[...])
    high_ref[...] = high
    low_ref[...] = low
    scale, more = scale_and_rest(cells_ref, rest_ref)
    wx_ref[0] = scale * (1.0 - cells_ref[2])
    wx_ref[1] = scale * cells_ref[2]

    def amplitude(t, out):
        row = lambda ref, n: ref[n, pl.ds(t, 1), :]
        wx = tent(half, row(cells_ref, 0), row(wx_ref, 0), row(wx_ref, 1))
        return [jnp.sum(part * wx, axis=0, keepdims=True) for part in (out[:half], out[half:])]

    def weights(t, low, high):
        return place(cell_masks(columns, cells_ref[1, pl.ds(t, 1), :]), low.astype(bf16), high.astype(bf16))

    def body(t, carry):
        wy = weights(t, cells_ref[4, pl.ds(t, 1), :], cells_ref[5, pl.ds(t, 1), :])
        amp = amplitude(t, dot2((high_ref[...], low_ref[...]), wy))
        amp_ref[0, pl.ds(t, 1), :], amp_ref[1, pl.ds(t, 1), :] = amp
        return carry

    lax.fori_loop(0, tiles, body, 0, unroll=math.gcd(tiles, BATCH))

    @pl.when(more)
    def _():
        def body(t, carry):
            wy = weights(t, rest_ref[0, pl.ds(t, 1), :], rest_ref[1, pl.ds(t, 1), :])
            amp = amplitude(t, dot(high_ref[...], wy))
            amp_ref[0, pl.ds(t, 1), :] += amp[0]
            amp_ref[1, pl.ds(t, 1), :] += amp[1]
            return carry

        lax.fori_loop(0, tiles, body, 0)


def pack_kernel(radiation_ref, electrons_ref, index_ref, offset_ref, out_ref):
    rows, slices, width = radiation_ref.shape
    tiles = electrons_ref.shape[2] // TILE
    for n in range(slices):
        out_ref[n, :rows, :] = radiation_ref[:, n, : width // 2]
        out_ref[n, rows : 2 * rows, :] = radiation_ref[:, n, width // 2 :]
        at = 2 * rows
        for ref in (electrons_ref, index_ref, offset_ref):
            for k in (0, 1):
                for t in range(tiles):
                    line = ref[k, n : n + 1, t * TILE : (t + 1) * TILE]
                    out_ref[n, at : at + 1, :] = line.astype(f32)
                    at += 1


def first_kernel(where_ref, *refs):
    *blocks, field_ref, amp_ref, state_ref, cells_ref, high_ref, low_ref, wx_ref, rest_ref = refs
    half = field_ref.shape[0] // 2
    count = len(blocks) // 2
    rows = half // len(blocks)
    tiles = cells_ref.shape[1] // count
    for n, ref in enumerate(blocks):
        at = pl.multiple_of(where_ref[n] * rows, rows)
        field_ref[pl.ds(at, rows), :] = ref[:rows, :]
        field_ref[pl.ds(half + at, rows), :] = ref[rows : 2 * rows, :]
        if n < count:
            for k in range(6):
                line = ref[2 * rows + k * tiles : 2 * rows + (k + 1) * tiles, :]
                target = state_ref.at[k] if k < 2 else cells_ref.at[k - 2]
                target[n * tiles : (n + 1) * tiles, :] = line
    cells_ref[4], cells_ref[5] = weight_pair(cells_ref[3])
    gather_tiles(field_ref, cells_ref, high_ref, low_ref, wx_ref, rest_ref, amp_ref)


def gather_kernel(fresh_ref, own_ref, other_ref, kx_ref, ky_ref, cells_ref, field_ref, amp_ref, *scratch):
    half = field_ref.shape[0] // 2
    moved = propagate(own_ref[...] + other_ref[...], kx_ref[...].reshape(2 * half, half), ky_ref)
    field_ref[...] = jnp.where(fresh_ref[0] == 1, 0.0, moved)
    gather_tiles(field_ref, cells_ref, *scratch, amp_ref)


def push_kernel(amp_ref, state_ref, cells_ref, field_ref, current_ref, out_ref, values_ref, rest_ref):
    half = current_ref.shape[0] // 2
    columns = current_ref.shape[1]
    phase = state_ref[0]
    energy = state_ref[1] - coupling * (amp_ref[0] * jnp.cos(phase) - amp_ref[1] * jnp.sin(phase))
    phase = phase + phase_step * energy
    out_ref[0] = phase
    out_ref[1] = energy
    scale, more = scale_and_rest(cells_ref, rest_ref)
    for part, factor in enumerate((jnp.cos(phase), -jnp.sin(phase))):
        for side, weight in enumerate((1.0 - cells_ref[2], cells_ref[2])):
            high, low = split((current_gain * scale) * weight * factor)
            values_ref[4 * part + side] = high.astype(f32)
            values_ref[4 * part + 2 + side] = low.astype(f32)
    current_ref[...] = 0.5 * field_ref[...]
    tiles = cells_ref.shape[1]
    batch = math.gcd(tiles, BATCH)

    def values(t, which):
        masks = cell_masks(half, cells_ref[0, pl.ds(t, 1), :])
        pair = lambda n: (values_ref[n + side, pl.ds(t, 1), :].astype(bf16) for side in (0, 1))
        return [jnp.concatenate([place(masks, *pair(n)) for n in (first, 4 + first)], axis=0) for first in which]

    def weights(t, low, high):
        return place(cell_masks(columns, cells_ref[1, pl.ds(t, 1), :]), low.astype(bf16), high.astype(bf16))

    def body(n, carry):
        built = []
        for t in [n * batch + k for k in range(batch)]:
            built.append(values(t, (0, 2)) + [weights(t, cells_ref[4, pl.ds(t, 1), :], cells_ref[5, pl.ds(t, 1), :])])
        high, low, wy = (jnp.concatenate(parts, axis=1) for parts in zip(*built))
        current_ref[...] += dot2((high, low), wy, dot_t)
        return carry

    lax.fori_loop(0, tiles // batch, body, 0)

    @pl.when(more)
    def _():
        def body(t, carry):
            wy = weights(t, rest_ref[0, pl.ds(t, 1), :], rest_ref[1, pl.ds(t, 1), :])
            current_ref[...] += dot_t(values(t, (0,))[0], wy)
            return carry

        lax.fori_loop(0, tiles, body, 0)


def last_kernel(where_ref, own_ref, other_ref, kx_ref, ky_ref, rows_ref):
    count, rows = rows_ref.shape[0], rows_ref.shape[1] // 2
    starts = [pl.multiple_of(where_ref[n] * rows, rows) for n in range(count)]
    block = jnp.concatenate([kx_ref[part, pl.ds(at, rows), :] for part in (0, 1) for at in starts], axis=0)
    moved = propagate(own_ref[...] + other_ref[...], block, ky_ref)
    for n in range(count):
        rows_ref[n, :rows] = moved[n * rows : (n + 1) * rows]
        rows_ref[n, rows:] = moved[(count + n) * rows : (count + n + 1) * rows]


vmem = pl.BlockSpec(memory_space=pltpu.VMEM)
smem = pl.BlockSpec(memory_space=pltpu.SMEM)


def call(kernel, inputs, outs, scratch, flops):
    shapes = [jax.ShapeDtypeStruct(shape, f32) for shape in outs]
    moved = sum(4 * array.size for array in inputs) + sum(4 * shape.size for shape in shapes)
    return pl.pallas_call(
        kernel,
        out_shape=shapes,
        in_specs=[smem if array.ndim == 1 else vmem for array in inputs],
        out_specs=[vmem] * len(outs),
        scratch_shapes=scratch,
        compiler_params=pltpu.CompilerParams(vmem_limit_bytes=VMEM_LIMIT),
        cost_estimate=pl.CostEstimate(flops=flops, bytes_accessed=moved, transcendentals=0),
    )(*inputs)


def shards(radiation, electrons, cell_index, cell_offset, kernel_x, kernel_y):
    cuts, dom = lax.axis_size("cuts"), lax.axis_size("dom")
    rows, slices, _ = radiation.shape
    half = kernel_x.shape[1]
    columns = kernel_y.shape[1]
    team = dom // slices
    groups = cuts * slices
    me = lax.axis_index("dom")
    mine = me // team
    cut = lax.axis_index("cuts")

    def seat(cut, number):
        return (1 - cut % 2) * number + (cut % 2) * (slices - 1 - number)

    def number(cut, team_number):
        return cut * slices + seat(cut, team_number)

    group = number(cut, mine)
    tiles = electrons.shape[2] // TILE

    def move(value, target):
        route = []
        for cut in range(cuts):
            for place in range(dom):
                to_cut, to_place = target(cut, place)
                route.append((cut * dom + place, to_cut * dom + to_place))
        return lax.ppermute(value, ("cuts", "dom"), route)

    def pick(array, which):
        return lax.dynamic_index_in_dim(array, which, 0, keepdims=False)

    def to_group(shift, turn=0):
        def target(cut, place):
            home = (number(cut, place // team) + shift) % groups
            return home // slices, seat(home // slices, (home + turn) % slices) * team + place % team

        return target

    def across(value):
        return move(value, lambda cut, place: (cut, place ^ 1))

    (payload,) = call(
        pack_kernel, [radiation, electrons, cell_index, cell_offset], [(slices, 2 * rows + 6 * tiles, columns)], [], 0
    )
    masks = range(0, dom, 2)
    own_blocks = []
    for mask in masks:
        block = pick(payload, seat(cut, (me ^ mask) // team))
        if mask:
            block = move(block, lambda cut, place: (cut, place ^ mask))
        own_blocks.append(block)
    other_blocks = [across(block[: 2 * rows]) for block in own_blocks]
    where = jnp.stack([me ^ mask for mask in masks] + [me ^ 1 ^ mask for mask in masks]).astype(jnp.int32)

    field_shape = (2 * half, columns)
    state_shape = (2, len(masks) * tiles, TILE)
    cells_shape = (6,) + state_shape[1:]
    pair = pltpu.VMEM(state_shape, f32)
    splits = [pltpu.VMEM(field_shape, bf16)] * 2 + [pair] * 2
    work = 4 * 2 * half * columns * state_shape[1] * TILE
    field, amp, state, cells = call(
        first_kernel,
        [where] + own_blocks + other_blocks,
        [field_shape, state_shape, state_shape, cells_shape],
        splits,
        work,
    )
    cells_of = [cells]
    for step in range(ITERS):
        if step > 0:
            fresh = ((group + step) % groups == 0).astype(jnp.int32).reshape(1)
            field, amp = call(
                gather_kernel,
                [fresh, own, other, kernel_x, kernel_y, cells_of[step]],
                [field_shape, state_shape],
                splits,
                work,
            )
        own, state = call(
            push_kernel,
            [amp, state, cells_of[step], field],
            [field_shape, state_shape],
            [pltpu.VMEM((8,) + state_shape[1:], f32), pair],
            work,
        )
        other = across(own)
        if step == 0:
            cells, _ = lax.optimization_barrier((cells, state))
            for later in range(1, ITERS):
                cells_of.append(move(cells, to_group(-later)))
        if step < ITERS - 1:
            state = move(state, to_group(-1))

    def places(home):
        return [seat(home // slices, (home + turn) % slices) * team + me % team for turn in range(slices)]

    field_home = (group + ITERS) % groups
    (blocks,) = call(
        last_kernel,
        [jnp.stack(places(field_home)).astype(jnp.int32), own, other, kernel_x, kernel_y],
        [(slices, 2 * rows, columns)],
        [],
        work // 16,
    )
    blocks, state = lax.optimization_barrier((blocks, state))
    landed = []
    for turn in range(slices):
        landed.append(move(blocks[turn], to_group(ITERS, turn)))
    state_home = (group + ITERS - 1) % groups
    seats = places(state_home)
    returned = []
    for turn in range(slices):
        chunk = (seats[turn] ^ seats[0]) // 2
        block = lax.dynamic_slice_in_dim(state, chunk * tiles, tiles, 1)
        returned.append(move(block, to_group(ITERS - 1, turn)))
    order = [(seat(cut, mine) - number) % slices for number in range(slices)]
    landed = jnp.stack(landed)
    landed = [pick(landed, which) for which in order]
    returned = jnp.stack(returned)
    returned = [pick(returned, which).reshape(2, tiles * TILE) for which in order]
    landed[0] = jnp.where(cut == 0, 0.0, landed[0])
    radiation_out = jnp.stack([jnp.concatenate([block[:rows], block[rows:]], axis=1) for block in landed], axis=1)
    return radiation_out, jnp.stack(returned, axis=1)


def solution(mesh):
    placed = (
        P("dom", "cuts", None),
        P(None, "cuts", "dom"),
        P(None, "cuts", "dom"),
        P(None, "cuts", "dom"),
        P(),
        P(),
    )

    return jax.shard_map(
        shards,
        mesh=mesh,
        in_specs=placed,
        out_specs=(P("dom", "cuts", None), P(None, "cuts", "dom")),
        check_vma=False,
    )
```

```python
import math

import jax
import jax.numpy as jnp
from jax import lax
from jax.experimental import pallas as pl
from jax.experimental.pallas import tpu as pltpu
from jax.sharding import PartitionSpec as P


ITERS = 4
TILE = 256
BATCH = 16
CHOICES = 64
REST = 1e-4
VMEM_LIMIT = 16 * 2**20

coupling = 0.5
phase_step = 1.0
current_gain = 1.0

f32 = jnp.float32
bf16 = jnp.bfloat16


def split(value):
    high = value.astype(bf16)
    return high, (value - high.astype(f32)).astype(bf16)


def dot(left, right):
    return jnp.dot(left, right, preferred_element_type=f32)


def dot_t(left, right):
    return lax.dot_general(left, right, (((1,), (1,)), ((), ())), preferred_element_type=f32)


def dot3(left, right, product=dot):
    return product(left[0], right[0]) + product(left[1], right[0]) + product(left[0], right[1])


def dot2(left, right, product=dot):
    return product(left[0], right) + product(left[1], right)


def tent(rows, index, low, high):
    cell = lax.broadcasted_iota(jnp.int32, (rows, index.shape[1]), 0).astype(f32)
    return jnp.where(cell == index, low, jnp.where(cell == index + 1.0, high, 0.0))


def weight_pair(offset):
    small = jnp.minimum(offset, 1.0 - offset)
    ratio = small / jnp.maximum(offset, 1.0 - offset)
    best = jnp.full_like(offset, 2.0)
    large = jnp.ones_like(offset)
    for n in range(CHOICES):
        choice = 1.0 + n / CHOICES
        other = choice * ratio
        miss = jnp.abs(other.astype(bf16).astype(f32) - other) * (1.0 / choice)
        large = jnp.where(miss < best, choice, large)
        best = jnp.minimum(miss, best)
    little = (large * ratio).astype(bf16).astype(f32)
    swap = offset > 0.5
    return jnp.where(swap, little, large), jnp.where(swap, large, little)


def scale_and_rest(cells_ref, rest_ref):
    offset, low, high = cells_ref[3], cells_ref[4], cells_ref[5]
    scale = ((1.0 - offset) * low + offset * high) / (low * low + high * high)
    rest_low = (1.0 - offset) - scale * low
    rest_high = offset - scale * high
    rest_ref[0] = rest_low / scale
    rest_ref[1] = rest_high / scale
    miss = jnp.sum(rest_low * rest_low + rest_high * rest_high)
    return scale, miss > (REST * REST) * 0.5 * offset.size


def complex_rows(real, imag):
    rows = real.shape[0] // 2
    return jnp.concatenate([real[:rows] - imag[rows:], real[rows:] + imag[:rows]], axis=0)


def propagate(field, kernel_x, kernel_y):
    half = field.shape[0] // 2
    left = split(kernel_x)
    mixed = split(complex_rows(dot3(left, split(field[:half])), dot3(left, split(field[half:]))))
    return complex_rows(dot3(mixed, split(kernel_y[0])), dot3(mixed, split(kernel_y[1])))


def cell_masks(rows, index):
    shape = (rows, index.shape[1])
    cell = lax.broadcasted_iota(jnp.int32, shape, 0).astype(f32).astype(bf16)
    at = lambda value: jnp.broadcast_to(value.astype(bf16), shape)
    return cell == at(index), cell == at(index + 1.0)


def place(masks, low, high):
    spread = lambda value: jnp.broadcast_to(value, masks[0].shape)
    return jnp.where(masks[0], spread(low), jnp.where(masks[1], spread(high), jnp.zeros(masks[0].shape, low.dtype)))


def gather_tiles(field_ref, cells_ref, high_ref, low_ref, wx_ref, rest_ref, amp_ref):
    half = field_ref.shape[0] // 2
    columns = field_ref.shape[1]
    tiles = cells_ref.shape[1]
    high, low = split(field_ref[...])
    high_ref[...] = high
    low_ref[...] = low
    scale, more = scale_and_rest(cells_ref, rest_ref)
    wx_ref[0] = scale * (1.0 - cells_ref[2])
    wx_ref[1] = scale * cells_ref[2]

    def amplitude(t, out):
        row = lambda ref, n: ref[n, pl.ds(t, 1), :]
        wx = tent(half, row(cells_ref, 0), row(wx_ref, 0), row(wx_ref, 1))
        return [jnp.sum(part * wx, axis=0, keepdims=True) for part in (out[:half], out[half:])]

    def weights(t, low, high):
        return place(cell_masks(columns, cells_ref[1, pl.ds(t, 1), :]), low.astype(bf16), high.astype(bf16))

    def body(t, carry):
        wy = weights(t, cells_ref[4, pl.ds(t, 1), :], cells_ref[5, pl.ds(t, 1), :])
        amp = amplitude(t, dot2((high_ref[...], low_ref[...]), wy))
        amp_ref[0, pl.ds(t, 1), :], amp_ref[1, pl.ds(t, 1), :] = amp
        return carry

    lax.fori_loop(0, tiles, body, 0, unroll=math.gcd(tiles, BATCH))

    @pl.when(more)
    def _():
        def body(t, carry):
            wy = weights(t, rest_ref[0, pl.ds(t, 1), :], rest_ref[1, pl.ds(t, 1), :])
            amp = amplitude(t, dot(high_ref[...], wy))
            amp_ref[0, pl.ds(t, 1), :] += amp[0]
            amp_ref[1, pl.ds(t, 1), :] += amp[1]
            return carry

        lax.fori_loop(0, tiles, body, 0)


def pack_kernel(radiation_ref, electrons_ref, index_ref, offset_ref, out_ref):
    rows, slices, width = radiation_ref.shape
    tiles = electrons_ref.shape[2] // TILE
    for n in range(slices):
        out_ref[n, :rows, :] = radiation_ref[:, n, : width // 2]
        out_ref[n, rows : 2 * rows, :] = radiation_ref[:, n, width // 2 :]
        at = 2 * rows
        for ref in (electrons_ref, index_ref, offset_ref):
            for k in (0, 1):
                for t in range(tiles):
                    line = ref[k, n : n + 1, t * TILE : (t + 1) * TILE]
                    out_ref[n, at : at + 1, :] = line.astype(f32)
                    at += 1


def lay_kernel(*refs):
    *blocks, state_ref, cells_ref = refs
    tiles = cells_ref.shape[1] // len(blocks)
    for n, ref in enumerate(blocks):
        above = ref.shape[0] - 6 * tiles
        for k in range(6):
            target = state_ref.at[k] if k < 2 else cells_ref.at[k - 2]
            target[n * tiles : (n + 1) * tiles, :] = ref[above + k * tiles : above + (k + 1) * tiles, :]
    cells_ref[4], cells_ref[5] = weight_pair(cells_ref[3])


def first_kernel(where_ref, cells_ref, *refs):
    *blocks, field_ref, amp_ref, high_ref, low_ref, wx_ref, rest_ref = refs
    half = field_ref.shape[0] // 2
    rows = half // len(blocks)
    for n, ref in enumerate(blocks):
        at = pl.multiple_of(where_ref[n] * rows, rows)
        field_ref[pl.ds(at, rows), :] = ref[:rows, :]
        field_ref[pl.ds(half + at, rows), :] = ref[rows : 2 * rows, :]
    gather_tiles(field_ref, cells_ref, high_ref, low_ref, wx_ref, rest_ref, amp_ref)


def gather_kernel(fresh_ref, own_ref, other_ref, kx_ref, ky_ref, cells_ref, field_ref, amp_ref, *scratch):
    half = field_ref.shape[0] // 2
    moved = propagate(own_ref[...] + other_ref[...], kx_ref[...].reshape(2 * half, half), ky_ref)
    field_ref[...] = jnp.where(fresh_ref[0] == 1, 0.0, moved)
    gather_tiles(field_ref, cells_ref, *scratch, amp_ref)


def push_kernel(amp_ref, state_ref, cells_ref, field_ref, current_ref, out_ref, values_ref, rest_ref):
    half = current_ref.shape[0] // 2
    columns = current_ref.shape[1]
    phase = state_ref[0]
    energy = state_ref[1] - coupling * (amp_ref[0] * jnp.cos(phase) - amp_ref[1] * jnp.sin(phase))
    phase = phase + phase_step * energy
    out_ref[0] = phase
    out_ref[1] = energy
    scale, more = scale_and_rest(cells_ref, rest_ref)
    for part, factor in enumerate((jnp.cos(phase), -jnp.sin(phase))):
        for side, weight in enumerate((1.0 - cells_ref[2], cells_ref[2])):
            high, low = split((current_gain * scale) * weight * factor)
            values_ref[4 * part + side] = high.astype(f32)
            values_ref[4 * part + 2 + side] = low.astype(f32)
    current_ref[...] = 0.5 * field_ref[...]
    tiles = cells_ref.shape[1]
    batch = math.gcd(tiles, BATCH)

    def values(t, which):
        masks = cell_masks(half, cells_ref[0, pl.ds(t, 1), :])
        pair = lambda n: (values_ref[n + side, pl.ds(t, 1), :].astype(bf16) for side in (0, 1))
        return [jnp.concatenate([place(masks, *pair(n)) for n in (first, 4 + first)], axis=0) for first in which]

    def weights(t, low, high):
        return place(cell_masks(columns, cells_ref[1, pl.ds(t, 1), :]), low.astype(bf16), high.astype(bf16))

    def body(n, carry):
        built = []
        for t in [n * batch + k for k in range(batch)]:
            built.append(values(t, (0, 2)) + [weights(t, cells_ref[4, pl.ds(t, 1), :], cells_ref[5, pl.ds(t, 1), :])])
        high, low, wy = (jnp.concatenate(parts, axis=1) for parts in zip(*built))
        current_ref[...] += dot2((high, low), wy, dot_t)
        return carry

    lax.fori_loop(0, tiles // batch, body, 0)

    @pl.when(more)
    def _():
        def body(t, carry):
            wy = weights(t, rest_ref[0, pl.ds(t, 1), :], rest_ref[1, pl.ds(t, 1), :])
            current_ref[...] += dot_t(values(t, (0,))[0], wy)
            return carry

        lax.fori_loop(0, tiles, body, 0)


def last_kernel(where_ref, own_ref, other_ref, kx_ref, ky_ref, rows_ref):
    count, rows = rows_ref.shape[0], rows_ref.shape[1] // 2
    starts = [pl.multiple_of(where_ref[n] * rows, rows) for n in range(count)]
    block = jnp.concatenate([kx_ref[part, pl.ds(at, rows), :] for part in (0, 1) for at in starts], axis=0)
    moved = propagate(own_ref[...] + other_ref[...], block, ky_ref)
    for n in range(count):
        rows_ref[n, :rows] = moved[n * rows : (n + 1) * rows]
        rows_ref[n, rows:] = moved[(count + n) * rows : (count + n + 1) * rows]


def final_kernel(order_ref, zero_ref, *refs):
    *blocks, radiation_ref, electrons_ref = refs
    rows, slices, width = radiation_ref.shape
    tiles = electrons_ref.shape[2] // TILE
    for n in range(slices):
        for turn in range(slices):

            @pl.when(order_ref[n] == turn)
            def _():
                block, state = blocks[turn], blocks[slices + turn]
                radiation_ref[:, n, : width // 2] = jnp.where(zero_ref[n] == 1, 0.0, block[:rows, :])
                radiation_ref[:, n, width // 2 :] = jnp.where(zero_ref[n] == 1, 0.0, block[rows:, :])
                for k in (0, 1):
                    for t in range(tiles):
                        electrons_ref[k, n : n + 1, t * TILE : (t + 1) * TILE] = state[k, t : t + 1, :]


vmem = pl.BlockSpec(memory_space=pltpu.VMEM)
smem = pl.BlockSpec(memory_space=pltpu.SMEM)


def call(kernel, inputs, outs, scratch, flops, limit=VMEM_LIMIT):
    shapes = [jax.ShapeDtypeStruct(shape, f32) for shape in outs]
    moved = sum(4 * array.size for array in inputs) + sum(4 * shape.size for shape in shapes)
    return pl.pallas_call(
        kernel,
        out_shape=shapes,
        in_specs=[smem if array.ndim == 1 else vmem for array in inputs],
        out_specs=[vmem] * len(outs),
        scratch_shapes=scratch,
        compiler_params=pltpu.CompilerParams(vmem_limit_bytes=limit),
        cost_estimate=pl.CostEstimate(flops=flops, bytes_accessed=moved, transcendentals=0),
    )(*inputs)


def shards(radiation, electrons, cell_index, cell_offset, kernel_x, kernel_y):
    cuts, dom = lax.axis_size("cuts"), lax.axis_size("dom")
    rows, slices, _ = radiation.shape
    half = kernel_x.shape[1]
    columns = kernel_y.shape[1]
    team = dom // slices
    groups = cuts * slices
    me = lax.axis_index("dom")
    mine = me // team
    cut = lax.axis_index("cuts")

    def seat(cut, number):
        return (1 - cut % 2) * number + (cut % 2) * (slices - 1 - number)

    def number(cut, team_number):
        return cut * slices + seat(cut, team_number)

    group = number(cut, mine)
    tiles = electrons.shape[2] // TILE

    def move(value, target):
        route = []
        for cut in range(cuts):
            for place in range(dom):
                to_cut, to_place = target(cut, place)
                route.append((cut * dom + place, to_cut * dom + to_place))
        return lax.ppermute(value, ("cuts", "dom"), route)

    def pick(array, which):
        return lax.dynamic_index_in_dim(array, which, 0, keepdims=False)

    def to_group(shift, turn=0):
        def target(cut, place):
            home = (number(cut, place // team) + shift) % groups
            return home // slices, seat(home // slices, (home + turn) % slices) * team + place % team

        return target

    def across(value):
        return move(value, lambda cut, place: (cut, place ^ 1))

    (payload,) = call(
        pack_kernel, [radiation, electrons, cell_index, cell_offset], [(slices, 2 * rows + 6 * tiles, columns)], [], 0
    )
    masks = range(0, dom, 2)
    own_blocks = []
    for mask in masks:
        block = pick(payload, seat(cut, (me ^ mask) // team))
        if mask:
            block = move(block, lambda cut, place: (cut, place ^ mask))
        own_blocks.append(block)
    other_blocks = []
    for block in own_blocks:
        other_blocks.append(across(block[: 2 * rows]))
    where = jnp.stack([me ^ mask for mask in masks] + [me ^ 1 ^ mask for mask in masks]).astype(jnp.int32)

    field_shape = (2 * half, columns)
    state_shape = (2, len(masks) * tiles, TILE)
    cells_shape = (6,) + state_shape[1:]
    pair = pltpu.VMEM(state_shape, f32)
    splits = [pltpu.VMEM(field_shape, bf16)] * 2 + [pair] * 2
    work = 4 * 2 * half * columns * state_shape[1] * TILE
    state, cells = call(lay_kernel, own_blocks, [state_shape, cells_shape], [], 0)
    cells_of = [cells]
    for later in range(1, ITERS):
        cells_of.append(move(cells, to_group(-later)))
    field, amp = call(
        first_kernel, [where, cells] + own_blocks + other_blocks, [field_shape, state_shape], splits, work
    )
    for step in range(ITERS):
        if step > 0:
            fresh = ((group + step) % groups == 0).astype(jnp.int32).reshape(1)
            field, amp = call(
                gather_kernel,
                [fresh, own, other, kernel_x, kernel_y, cells_of[step]],
                [field_shape, state_shape],
                splits,
                work,
            )
        own, state = call(
            push_kernel,
            [amp, state, cells_of[step], field],
            [field_shape, state_shape],
            [pltpu.VMEM((8,) + state_shape[1:], f32), pair],
            work,
        )
        other = across(own)
        if step < ITERS - 1:
            state = move(state, to_group(-1))

    def places(home):
        return [seat(home // slices, (home + turn) % slices) * team + me % team for turn in range(slices)]

    field_home = (group + ITERS) % groups
    (blocks,) = call(
        last_kernel,
        [jnp.stack(places(field_home)).astype(jnp.int32), own, other, kernel_x, kernel_y],
        [(slices, 2 * rows, columns)],
        [],
        work // 16,
    )
    blocks, state = lax.optimization_barrier((blocks, state))
    landed = []
    for turn in range(slices):
        landed.append(move(blocks[turn], to_group(ITERS, turn)))
    state_home = (group + ITERS - 1) % groups
    seats = places(state_home)
    returned = []
    for turn in range(slices):
        chunk = (seats[turn] ^ seats[0]) // 2
        block = lax.dynamic_slice_in_dim(state, chunk * tiles, tiles, 1)
        returned.append(move(block, to_group(ITERS - 1, turn)))
    order = jnp.stack([(seat(cut, mine) - n) % slices for n in range(slices)]).astype(jnp.int32)
    zero = jnp.stack([group - seat(cut, mine) + n == 0 for n in range(slices)]).astype(jnp.int32)
    return tuple(call(final_kernel, [order, zero] + landed + returned, [radiation.shape, electrons.shape], [], 0))


def solution(mesh):
    placed = (
        P("dom", "cuts", None),
        P(None, "cuts", "dom"),
        P(None, "cuts", "dom"),
        P(None, "cuts", "dom"),
        P(),
        P(),
    )

    return jax.shard_map(
        shards,
        mesh=mesh,
        in_specs=placed,
        out_specs=(P("dom", "cuts", None), P(None, "cuts", "dom")),
        check_vma=False,
    )
```

```python
import math

import jax
import jax.numpy as jnp
from jax import lax
from jax.experimental import pallas as pl
from jax.experimental.pallas import tpu as pltpu
from jax.sharding import PartitionSpec as P


ITERS = 4
TILE = 256
BATCH = 16
CHOICES = 64
REST = 1e-4
VMEM_LIMIT = 16 * 2**20

coupling = 0.5
phase_step = 1.0
current_gain = 1.0

f32 = jnp.float32
bf16 = jnp.bfloat16


def split(value):
    high = value.astype(bf16)
    return high, (value - high.astype(f32)).astype(bf16)


def dot(left, right):
    return jnp.dot(left, right, preferred_element_type=f32)


def dot_t(left, right):
    return lax.dot_general(left, right, (((1,), (1,)), ((), ())), preferred_element_type=f32)


def dot3(left, right, product=dot):
    return product(left[0], right[0]) + product(left[1], right[0]) + product(left[0], right[1])


def dot2(left, right, product=dot):
    return product(left[0], right) + product(left[1], right)


def tent(rows, index, low, high):
    cell = lax.broadcasted_iota(jnp.int32, (rows, index.shape[1]), 0).astype(f32)
    return jnp.where(cell == index, low, jnp.where(cell == index + 1.0, high, 0.0))


def weight_pair(offset):
    small = jnp.minimum(offset, 1.0 - offset)
    ratio = small / jnp.maximum(offset, 1.0 - offset)
    best = jnp.full_like(offset, 2.0)
    large = jnp.ones_like(offset)
    for n in range(CHOICES):
        choice = 1.0 + n / CHOICES
        other = choice * ratio
        miss = jnp.abs(other.astype(bf16).astype(f32) - other) * (1.0 / choice)
        large = jnp.where(miss < best, choice, large)
        best = jnp.minimum(miss, best)
    little = (large * ratio).astype(bf16).astype(f32)
    swap = offset > 0.5
    return jnp.where(swap, little, large), jnp.where(swap, large, little)


def scale_and_rest(cells_ref, rest_ref):
    offset, low, high = cells_ref[3], cells_ref[4], cells_ref[5]
    scale = ((1.0 - offset) * low + offset * high) / (low * low + high * high)
    rest_low = (1.0 - offset) - scale * low
    rest_high = offset - scale * high
    rest_ref[0] = rest_low / scale
    rest_ref[1] = rest_high / scale
    miss = jnp.sum(rest_low * rest_low + rest_high * rest_high)
    return scale, miss > (REST * REST) * 0.5 * offset.size


def parts_kernel(kx_ref, ky_ref, *outs):
    for ref, out_ref in zip((kx_ref, ky_ref), outs):
        for n, value in enumerate((ref[0], ref[1], ref[0] + ref[1])):
            out_ref[2 * n], out_ref[2 * n + 1] = split(value)


def complex_product(left, right):
    real, imag, both = (dot3(*pair) for pair in zip(left, right))
    return real - imag, both - real - imag


def triple(real, imag):
    return split(real), split(imag), split(real + imag)


def propagate(field, kernel_x, ky_ref):
    half = field.shape[0] // 2
    right = [(ky_ref[2 * n], ky_ref[2 * n + 1]) for n in range(3)]
    mixed = complex_product(kernel_x, triple(field[:half], field[half:]))
    return jnp.concatenate(complex_product(triple(*mixed), right), axis=0)


def cell_masks(rows, index):
    shape = (rows, index.shape[1])
    cell = lax.broadcasted_iota(jnp.int32, shape, 0).astype(f32).astype(bf16)
    at = lambda value: jnp.broadcast_to(value.astype(bf16), shape)
    return cell == at(index), cell == at(index + 1.0)


def place(masks, low, high):
    spread = lambda value: jnp.broadcast_to(value, masks[0].shape)
    return jnp.where(masks[0], spread(low), jnp.where(masks[1], spread(high), jnp.zeros(masks[0].shape, low.dtype)))


def gather_tiles(field_ref, cells_ref, high_ref, low_ref, wx_ref, rest_ref, amp_ref):
    half = field_ref.shape[0] // 2
    columns = field_ref.shape[1]
    tiles = cells_ref.shape[1]
    high, low = split(field_ref[...])
    high_ref[...] = high
    low_ref[...] = low
    scale, more = scale_and_rest(cells_ref, rest_ref)
    wx_ref[0] = scale * (1.0 - cells_ref[2])
    wx_ref[1] = scale * cells_ref[2]

    def amplitude(t, out):
        row = lambda ref, n: ref[n, pl.ds(t, 1), :]
        wx = tent(half, row(cells_ref, 0), row(wx_ref, 0), row(wx_ref, 1))
        return [jnp.sum(part * wx, axis=0, keepdims=True) for part in (out[:half], out[half:])]

    def weights(t, low, high):
        return place(cell_masks(columns, cells_ref[1, pl.ds(t, 1), :]), low.astype(bf16), high.astype(bf16))

    def body(t, carry):
        wy = weights(t, cells_ref[4, pl.ds(t, 1), :], cells_ref[5, pl.ds(t, 1), :])
        amp = amplitude(t, dot2((high_ref[...], low_ref[...]), wy))
        amp_ref[0, pl.ds(t, 1), :], amp_ref[1, pl.ds(t, 1), :] = amp
        return carry

    lax.fori_loop(0, tiles, body, 0, unroll=math.gcd(tiles, 2 * BATCH))

    @pl.when(more)
    def _():
        def body(t, carry):
            wy = weights(t, rest_ref[0, pl.ds(t, 1), :], rest_ref[1, pl.ds(t, 1), :])
            amp = amplitude(t, dot(high_ref[...], wy))
            amp_ref[0, pl.ds(t, 1), :] += amp[0]
            amp_ref[1, pl.ds(t, 1), :] += amp[1]
            return carry

        lax.fori_loop(0, tiles, body, 0)


def pack_kernel(radiation_ref, electrons_ref, index_ref, offset_ref, out_ref):
    rows, slices, width = radiation_ref.shape
    tiles = electrons_ref.shape[2] // TILE
    for n in range(slices):
        out_ref[n, :rows, :] = radiation_ref[:, n, : width // 2]
        out_ref[n, rows : 2 * rows, :] = radiation_ref[:, n, width // 2 :]
        at = 2 * rows
        for ref in (electrons_ref, index_ref, offset_ref):
            for k in (0, 1):
                for t in range(tiles):
                    line = ref[k, n : n + 1, t * TILE : (t + 1) * TILE]
                    out_ref[n, at : at + 1, :] = line.astype(f32)
                    at += 1


def lay_kernel(*refs):
    *blocks, state_ref, cells_ref = refs
    tiles = cells_ref.shape[1] // len(blocks)
    for n, ref in enumerate(blocks):
        above = ref.shape[0] - 6 * tiles
        for k in range(6):
            target = state_ref.at[k] if k < 2 else cells_ref.at[k - 2]
            target[n * tiles : (n + 1) * tiles, :] = ref[above + k * tiles : above + (k + 1) * tiles, :]
    cells_ref[4], cells_ref[5] = weight_pair(cells_ref[3])


def first_kernel(where_ref, cells_ref, *refs):
    *blocks, field_ref, amp_ref, high_ref, low_ref, wx_ref, rest_ref = refs
    half = field_ref.shape[0] // 2
    rows = half // len(blocks)
    for n, ref in enumerate(blocks):
        at = pl.multiple_of(where_ref[n] * rows, rows)
        field_ref[pl.ds(at, rows), :] = ref[:rows, :]
        field_ref[pl.ds(half + at, rows), :] = ref[rows : 2 * rows, :]
    gather_tiles(field_ref, cells_ref, high_ref, low_ref, wx_ref, rest_ref, amp_ref)


def gather_kernel(fresh_ref, own_ref, other_ref, kx_ref, ky_ref, cells_ref, field_ref, amp_ref, *scratch):
    left = [(kx_ref[2 * n], kx_ref[2 * n + 1]) for n in range(3)]
    moved = propagate(own_ref[...] + other_ref[...], left, ky_ref)
    field_ref[...] = jnp.where(fresh_ref[0] == 1, 0.0, moved)
    gather_tiles(field_ref, cells_ref, *scratch, amp_ref)


def push_kernel(amp_ref, state_ref, cells_ref, field_ref, current_ref, out_ref, values_ref, rest_ref):
    half = current_ref.shape[0] // 2
    columns = current_ref.shape[1]
    phase = state_ref[0]
    energy = state_ref[1] - coupling * (amp_ref[0] * jnp.cos(phase) - amp_ref[1] * jnp.sin(phase))
    phase = phase + phase_step * energy
    out_ref[0] = phase
    out_ref[1] = energy
    scale, more = scale_and_rest(cells_ref, rest_ref)
    for part, factor in enumerate((jnp.cos(phase), -jnp.sin(phase))):
        for side, weight in enumerate((1.0 - cells_ref[2], cells_ref[2])):
            high, low = split((current_gain * scale) * weight * factor)
            values_ref[4 * part + side] = high.astype(f32)
            values_ref[4 * part + 2 + side] = low.astype(f32)
    current_ref[...] = 0.5 * field_ref[...]
    tiles = cells_ref.shape[1]
    batch = math.gcd(tiles, BATCH)

    def values(t, which):
        masks = cell_masks(half, cells_ref[0, pl.ds(t, 1), :])
        pair = lambda n: (values_ref[n + side, pl.ds(t, 1), :].astype(bf16) for side in (0, 1))
        return [jnp.concatenate([place(masks, *pair(n)) for n in (first, 4 + first)], axis=0) for first in which]

    def weights(t, low, high):
        return place(cell_masks(columns, cells_ref[1, pl.ds(t, 1), :]), low.astype(bf16), high.astype(bf16))

    def body(n, carry):
        built = []
        for t in [n * batch + k for k in range(batch)]:
            built.append(values(t, (0, 2)) + [weights(t, cells_ref[4, pl.ds(t, 1), :], cells_ref[5, pl.ds(t, 1), :])])
        high, low, wy = (jnp.concatenate(parts, axis=1) for parts in zip(*built))
        current_ref[...] += dot2((high, low), wy, dot_t)
        return carry

    lax.fori_loop(0, tiles // batch, body, 0)

    @pl.when(more)
    def _():
        def body(t, carry):
            wy = weights(t, rest_ref[0, pl.ds(t, 1), :], rest_ref[1, pl.ds(t, 1), :])
            current_ref[...] += dot_t(values(t, (0,))[0], wy)
            return carry

        lax.fori_loop(0, tiles, body, 0)


def last_kernel(where_ref, own_ref, other_ref, kx_ref, ky_ref, rows_ref):
    count, rows = rows_ref.shape[0], rows_ref.shape[1] // 2
    starts = [pl.multiple_of(where_ref[n] * rows, rows) for n in range(count)]
    take = lambda part: jnp.concatenate([kx_ref[part, pl.ds(at, rows), :] for at in starts], axis=0)
    block = [(take(2 * n), take(2 * n + 1)) for n in range(3)]
    moved = propagate(own_ref[...] + other_ref[...], block, ky_ref)
    for n in range(count):
        rows_ref[n, :rows] = moved[n * rows : (n + 1) * rows]
        rows_ref[n, rows:] = moved[(count + n) * rows : (count + n + 1) * rows]


def final_kernel(order_ref, zero_ref, *refs):
    *blocks, radiation_ref, electrons_ref = refs
    rows, slices, width = radiation_ref.shape
    tiles = electrons_ref.shape[2] // TILE
    for n in range(slices):
        for turn in range(slices):

            @pl.when(order_ref[n] == turn)
            def _():
                block, state = blocks[turn], blocks[slices + turn]
                radiation_ref[:, n, : width // 2] = jnp.where(zero_ref[n] == 1, 0.0, block[:rows, :])
                radiation_ref[:, n, width // 2 :] = jnp.where(zero_ref[n] == 1, 0.0, block[rows:, :])
                for k in (0, 1):
                    for t in range(tiles):
                        electrons_ref[k, n : n + 1, t * TILE : (t + 1) * TILE] = state[k, t : t + 1, :]


vmem = pl.BlockSpec(memory_space=pltpu.VMEM)
smem = pl.BlockSpec(memory_space=pltpu.SMEM)


def call(kernel, inputs, outs, scratch, flops, limit=VMEM_LIMIT):
    shapes = [jax.ShapeDtypeStruct(shape, f32) if isinstance(shape, tuple) else shape for shape in outs]
    moved = sum(4 * array.size for array in inputs) + sum(4 * shape.size for shape in shapes)
    return pl.pallas_call(
        kernel,
        out_shape=shapes,
        in_specs=[smem if array.ndim == 1 else vmem for array in inputs],
        out_specs=[vmem] * len(outs),
        scratch_shapes=scratch,
        compiler_params=pltpu.CompilerParams(vmem_limit_bytes=limit),
        cost_estimate=pl.CostEstimate(flops=flops, bytes_accessed=moved, transcendentals=0),
    )(*inputs)


def shards(radiation, electrons, cell_index, cell_offset, kernel_x, kernel_y):
    cuts, dom = lax.axis_size("cuts"), lax.axis_size("dom")
    rows, slices, _ = radiation.shape
    half = kernel_x.shape[1]
    columns = kernel_y.shape[1]
    team = dom // slices
    groups = cuts * slices
    me = lax.axis_index("dom")
    mine = me // team
    cut = lax.axis_index("cuts")

    def seat(cut, number):
        return (1 - cut % 2) * number + (cut % 2) * (slices - 1 - number)

    def number(cut, team_number):
        return cut * slices + seat(cut, team_number)

    group = number(cut, mine)
    tiles = electrons.shape[2] // TILE

    def move(value, target):
        route = []
        for cut in range(cuts):
            for place in range(dom):
                to_cut, to_place = target(cut, place)
                route.append((cut * dom + place, to_cut * dom + to_place))
        return lax.ppermute(value, ("cuts", "dom"), route)

    def pick(array, which):
        return lax.dynamic_index_in_dim(array, which, 0, keepdims=False)

    def to_group(shift, turn=0):
        def target(cut, place):
            home = (number(cut, place // team) + shift) % groups
            return home // slices, seat(home // slices, (home + turn) % slices) * team + place % team

        return target

    def across(value):
        return move(value, lambda cut, place: (cut, place ^ 1))

    (payload,) = call(
        pack_kernel, [radiation, electrons, cell_index, cell_offset], [(slices, 2 * rows + 6 * tiles, columns)], [], 0
    )
    kx_parts, ky_parts = call(
        parts_kernel, [kernel_x, kernel_y], [jax.ShapeDtypeStruct((6,) + kernel_x.shape[1:], bf16)] * 2, [], 0
    )
    masks = range(0, dom, 2)
    own_blocks = []
    for mask in masks:
        block = pick(payload, seat(cut, (me ^ mask) // team))
        if mask:
            block = move(block, lambda cut, place: (cut, place ^ mask))
        own_blocks.append(block)
    other_blocks = []
    for block in own_blocks:
        other_blocks.append(across(block[: 2 * rows]))
    where = jnp.stack([me ^ mask for mask in masks] + [me ^ 1 ^ mask for mask in masks]).astype(jnp.int32)

    field_shape = (2 * half, columns)
    state_shape = (2, len(masks) * tiles, TILE)
    cells_shape = (6,) + state_shape[1:]
    pair = pltpu.VMEM(state_shape, f32)
    splits = [pltpu.VMEM(field_shape, bf16)] * 2 + [pair] * 2
    work = 4 * 2 * half * columns * state_shape[1] * TILE
    state, cells = call(lay_kernel, own_blocks, [state_shape, cells_shape], [], 0)
    cells_of = [cells]
    for later in range(1, ITERS):
        cells_of.append(move(cells, to_group(-later)))
    field, amp = call(
        first_kernel, [where, cells] + own_blocks + other_blocks, [field_shape, state_shape], splits, work
    )
    for step in range(ITERS):
        if step > 0:
            fresh = ((group + step) % groups == 0).astype(jnp.int32).reshape(1)
            field, amp = call(
                gather_kernel,
                [fresh, own, other, kx_parts, ky_parts, cells_of[step]],
                [field_shape, state_shape],
                splits,
                work,
            )
        own, state = call(
            push_kernel,
            [amp, state, cells_of[step], field],
            [field_shape, state_shape],
            [pltpu.VMEM((8,) + state_shape[1:], f32), pair],
            work,
        )
        other = across(own)
        if step < ITERS - 1:
            state = move(state, to_group(-1))

    def places(home):
        return [seat(home // slices, (home + turn) % slices) * team + me % team for turn in range(slices)]

    field_home = (group + ITERS) % groups
    (blocks,) = call(
        last_kernel,
        [jnp.stack(places(field_home)).astype(jnp.int32), own, other, kx_parts, ky_parts],
        [(slices, 2 * rows, columns)],
        [],
        work // 16,
    )
    blocks, state = lax.optimization_barrier((blocks, state))
    landed = []
    for turn in range(slices):
        landed.append(move(blocks[turn], to_group(ITERS, turn)))
    state_home = (group + ITERS - 1) % groups
    seats = places(state_home)
    returned = []
    for turn in range(slices):
        chunk = (seats[turn] ^ seats[0]) // 2
        block = lax.dynamic_slice_in_dim(state, chunk * tiles, tiles, 1)
        returned.append(move(block, to_group(ITERS - 1, turn)))
    order = jnp.stack([(seat(cut, mine) - n) % slices for n in range(slices)]).astype(jnp.int32)
    zero = jnp.stack([group - seat(cut, mine) + n == 0 for n in range(slices)]).astype(jnp.int32)
    return tuple(call(final_kernel, [order, zero] + landed + returned, [radiation.shape, electrons.shape], [], 0))


def solution(mesh):
    placed = (
        P("dom", "cuts", None),
        P(None, "cuts", "dom"),
        P(None, "cuts", "dom"),
        P(None, "cuts", "dom"),
        P(),
        P(),
    )

    return jax.shard_map(
        shards,
        mesh=mesh,
        in_specs=placed,
        out_specs=(P("dom", "cuts", None), P(None, "cuts", "dom")),
        check_vma=False,
    )
```

```python
import math

import jax
import jax.numpy as jnp
from jax import lax
from jax.experimental import pallas as pl
from jax.experimental.pallas import tpu as pltpu
from jax.sharding import PartitionSpec as P


ITERS = 4
TILE = 256
BATCH = 16
CHOICES = 64
REST = 1e-4
VMEM_LIMIT = 16 * 2**20

coupling = 0.5
phase_step = 1.0
current_gain = 1.0

f32 = jnp.float32
bf16 = jnp.bfloat16


def split(value):
    high = value.astype(bf16)
    return high, (value - high.astype(f32)).astype(bf16)


def dot(left, right):
    return jnp.dot(left, right, preferred_element_type=f32)


def dot_t(left, right):
    return lax.dot_general(left, right, (((1,), (1,)), ((), ())), preferred_element_type=f32)


def dot3(left, right, product=dot):
    return product(left[0], right[0]) + product(left[1], right[0]) + product(left[0], right[1])


def dot2(left, right, product=dot):
    return product(left[0], right) + product(left[1], right)


def tent(rows, index, low, high):
    cell = lax.broadcasted_iota(jnp.int32, (rows, index.shape[1]), 0).astype(f32)
    return jnp.where(cell == index, low, jnp.where(cell == index + 1.0, high, 0.0))


def weight_pair(offset):
    small = jnp.minimum(offset, 1.0 - offset)
    ratio = small / jnp.maximum(offset, 1.0 - offset)
    best = jnp.full_like(offset, 2.0)
    large = jnp.ones_like(offset)
    for n in range(CHOICES):
        choice = 1.0 + n / CHOICES
        other = choice * ratio
        miss = jnp.abs(other.astype(bf16).astype(f32) - other) * (1.0 / choice)
        large = jnp.where(miss < best, choice, large)
        best = jnp.minimum(miss, best)
    little = (large * ratio).astype(bf16).astype(f32)
    swap = offset > 0.5
    return jnp.where(swap, little, large), jnp.where(swap, large, little)


def scale_and_rest(cells_ref, rest_ref):
    offset, low, high = cells_ref[3], cells_ref[4], cells_ref[5]
    scale = ((1.0 - offset) * low + offset * high) / (low * low + high * high)
    rest_low = (1.0 - offset) - scale * low
    rest_high = offset - scale * high
    rest_ref[0] = rest_low / scale
    rest_ref[1] = rest_high / scale
    miss = jnp.sum(rest_low * rest_low + rest_high * rest_high)
    return scale, miss > (REST * REST) * 0.5 * offset.size


def parts_kernel(kx_ref, ky_ref, *outs):
    for ref, out_ref in zip((kx_ref, ky_ref), outs):
        for n, value in enumerate((ref[0], ref[1], ref[0] + ref[1])):
            out_ref[2 * n], out_ref[2 * n + 1] = split(value)


def complex_product(left, right):
    real, imag, both = (dot3(*pair) for pair in zip(left, right))
    return real - imag, both - real - imag


def triple(real, imag):
    return split(real), split(imag), split(real + imag)


def propagate(field, kernel_x, ky_ref):
    half = field.shape[0] // 2
    right = [(ky_ref[2 * n], ky_ref[2 * n + 1]) for n in range(3)]
    mixed = complex_product(kernel_x, triple(field[:half], field[half:]))
    return jnp.concatenate(complex_product(triple(*mixed), right), axis=0)


def cell_masks(rows, index):
    shape = (rows, index.shape[1])
    cell = lax.broadcasted_iota(jnp.int32, shape, 0).astype(f32).astype(bf16)
    at = lambda value: jnp.broadcast_to(value.astype(bf16), shape)
    return cell == at(index), cell == at(index + 1.0)


def place(masks, low, high):
    spread = lambda value: jnp.broadcast_to(value, masks[0].shape)
    return jnp.where(masks[0], spread(low), jnp.where(masks[1], spread(high), jnp.zeros(masks[0].shape, low.dtype)))


def gather_tiles(field_ref, cells_ref, high_ref, low_ref, wx_ref, rest_ref, amp_ref):
    half = field_ref.shape[0] // 2
    columns = field_ref.shape[1]
    tiles = cells_ref.shape[1]
    high, low = split(field_ref[...])
    high_ref[...] = high
    low_ref[...] = low
    scale, more = scale_and_rest(cells_ref, rest_ref)
    wx_ref[0] = scale * (1.0 - cells_ref[2])
    wx_ref[1] = scale * cells_ref[2]

    def amplitude(t, out):
        row = lambda ref, n: ref[n, pl.ds(t, 1), :]
        wx = tent(half, row(cells_ref, 0), row(wx_ref, 0), row(wx_ref, 1))
        return [jnp.sum(part * wx, axis=0, keepdims=True) for part in (out[:half], out[half:])]

    def weights(t, low, high):
        return place(cell_masks(columns, cells_ref[1, pl.ds(t, 1), :]), low.astype(bf16), high.astype(bf16))

    def body(t, carry):
        wy = weights(t, cells_ref[4, pl.ds(t, 1), :], cells_ref[5, pl.ds(t, 1), :])
        amp = amplitude(t, dot2((high_ref[...], low_ref[...]), wy))
        amp_ref[0, pl.ds(t, 1), :], amp_ref[1, pl.ds(t, 1), :] = amp
        return carry

    lax.fori_loop(0, tiles, body, 0, unroll=math.gcd(tiles, 2 * BATCH))

    @pl.when(more)
    def _():
        def body(t, carry):
            wy = weights(t, rest_ref[0, pl.ds(t, 1), :], rest_ref[1, pl.ds(t, 1), :])
            amp = amplitude(t, dot(high_ref[...], wy))
            amp_ref[0, pl.ds(t, 1), :] += amp[0]
            amp_ref[1, pl.ds(t, 1), :] += amp[1]
            return carry

        lax.fori_loop(0, tiles, body, 0)


def pack_kernel(radiation_ref, electrons_ref, index_ref, offset_ref, out_ref):
    rows, slices, width = radiation_ref.shape
    tiles = electrons_ref.shape[2] // TILE
    for n in range(slices):
        out_ref[n, :rows, :] = radiation_ref[:, n, : width // 2]
        out_ref[n, rows : 2 * rows, :] = radiation_ref[:, n, width // 2 :]
        at = 2 * rows
        for ref in (electrons_ref, index_ref, offset_ref):
            for k in (0, 1):
                for t in range(tiles):
                    line = ref[k, n : n + 1, t * TILE : (t + 1) * TILE]
                    out_ref[n, at : at + 1, :] = line.astype(f32)
                    at += 1


def lay_kernel(*refs):
    *blocks, state_ref, cells_ref = refs
    tiles = cells_ref.shape[1] // len(blocks)
    for n, ref in enumerate(blocks):
        above = ref.shape[0] - 6 * tiles
        for k in range(6):
            target = state_ref.at[k] if k < 2 else cells_ref.at[k - 2]
            target[n * tiles : (n + 1) * tiles, :] = ref[above + k * tiles : above + (k + 1) * tiles, :]
    cells_ref[4], cells_ref[5] = weight_pair(cells_ref[3])


def first_kernel(where_ref, cells_ref, *refs):
    *blocks, field_ref, amp_ref, high_ref, low_ref, wx_ref, rest_ref = refs
    half = field_ref.shape[0] // 2
    rows = half // len(blocks)
    for n, ref in enumerate(blocks):
        at = pl.multiple_of(where_ref[n] * rows, rows)
        field_ref[pl.ds(at, rows), :] = ref[:rows, :]
        field_ref[pl.ds(half + at, rows), :] = ref[rows : 2 * rows, :]
    gather_tiles(field_ref, cells_ref, high_ref, low_ref, wx_ref, rest_ref, amp_ref)


def gather_kernel(fresh_ref, own_ref, other_ref, kx_ref, ky_ref, cells_ref, field_ref, amp_ref, *scratch):
    left = [(kx_ref[2 * n], kx_ref[2 * n + 1]) for n in range(3)]
    moved = propagate(own_ref[...] + other_ref[...], left, ky_ref)
    field_ref[...] = jnp.where(fresh_ref[0] == 1, 0.0, moved)
    gather_tiles(field_ref, cells_ref, *scratch, amp_ref)


def push_kernel(amp_ref, state_ref, cells_ref, field_ref, current_ref, out_ref, values_ref, rest_ref):
    half = current_ref.shape[0] // 2
    columns = current_ref.shape[1]
    phase = state_ref[0]
    energy = state_ref[1] - coupling * (amp_ref[0] * jnp.cos(phase) - amp_ref[1] * jnp.sin(phase))
    phase = phase + phase_step * energy
    out_ref[0] = phase
    out_ref[1] = energy
    scale, more = scale_and_rest(cells_ref, rest_ref)
    for part, factor in enumerate((jnp.cos(phase), -jnp.sin(phase))):
        for side, weight in enumerate((1.0 - cells_ref[2], cells_ref[2])):
            high, low = split((current_gain * scale) * weight * factor)
            values_ref[4 * part + side] = high.astype(f32)
            values_ref[4 * part + 2 + side] = low.astype(f32)
    current_ref[...] = 0.5 * field_ref[...]
    tiles = cells_ref.shape[1]
    batch = math.gcd(tiles, BATCH)

    def values(t, which):
        masks = cell_masks(half, cells_ref[0, pl.ds(t, 1), :])
        pair = lambda n: (values_ref[n + side, pl.ds(t, 1), :].astype(bf16) for side in (0, 1))
        return [jnp.concatenate([place(masks, *pair(n)) for n in (first, 4 + first)], axis=0) for first in which]

    def weights(t, low, high):
        return place(cell_masks(columns, cells_ref[1, pl.ds(t, 1), :]), low.astype(bf16), high.astype(bf16))

    def body(n, carry):
        built = []
        for t in [n * batch + k for k in range(batch)]:
            built.append(values(t, (0, 2)) + [weights(t, cells_ref[4, pl.ds(t, 1), :], cells_ref[5, pl.ds(t, 1), :])])
        high, low, wy = (jnp.concatenate(parts, axis=1) for parts in zip(*built))
        current_ref[...] += dot2((high, low), wy, dot_t)
        return carry

    lax.fori_loop(0, tiles // batch, body, 0)

    @pl.when(more)
    def _():
        def body(t, carry):
            wy = weights(t, rest_ref[0, pl.ds(t, 1), :], rest_ref[1, pl.ds(t, 1), :])
            current_ref[...] += dot_t(values(t, (0,))[0], wy)
            return carry

        lax.fori_loop(0, tiles, body, 0)


def last_kernel(where_ref, own_ref, other_ref, kx_ref, ky_ref, rows_ref):
    count, rows = rows_ref.shape[0], rows_ref.shape[1] // 2
    starts = [pl.multiple_of(where_ref[n] * rows, rows) for n in range(count)]
    take = lambda part: jnp.concatenate([kx_ref[part, pl.ds(at, rows), :] for at in starts], axis=0)
    block = [(take(2 * n), take(2 * n + 1)) for n in range(3)]
    moved = propagate(own_ref[...] + other_ref[...], block, ky_ref)
    for n in range(count):
        rows_ref[n, :rows] = moved[n * rows : (n + 1) * rows]
        rows_ref[n, rows:] = moved[(count + n) * rows : (count + n + 1) * rows]


def final_kernel(order_ref, zero_ref, *refs):
    *blocks, radiation_ref, electrons_ref = refs
    rows, slices, width = radiation_ref.shape
    tiles = electrons_ref.shape[2] // TILE
    for n in range(slices):
        for turn in range(slices):

            @pl.when(order_ref[n] == turn)
            def _():
                block, state = blocks[turn], blocks[slices + turn]
                radiation_ref[:, n, : width // 2] = jnp.where(zero_ref[n] == 1, 0.0, block[:rows, :])
                radiation_ref[:, n, width // 2 :] = jnp.where(zero_ref[n] == 1, 0.0, block[rows:, :])
                for k in (0, 1):
                    for t in range(tiles):
                        electrons_ref[k, n : n + 1, t * TILE : (t + 1) * TILE] = state[k, t : t + 1, :]


vmem = pl.BlockSpec(memory_space=pltpu.VMEM)
smem = pl.BlockSpec(memory_space=pltpu.SMEM)


def call(kernel, inputs, outs, scratch, flops, limit=VMEM_LIMIT):
    shapes = [jax.ShapeDtypeStruct(shape, f32) if isinstance(shape, tuple) else shape for shape in outs]
    moved = sum(4 * array.size for array in inputs) + sum(4 * shape.size for shape in shapes)
    return pl.pallas_call(
        kernel,
        out_shape=shapes,
        in_specs=[smem if array.ndim == 1 else vmem for array in inputs],
        out_specs=[vmem] * len(outs),
        scratch_shapes=scratch,
        compiler_params=pltpu.CompilerParams(vmem_limit_bytes=limit),
        cost_estimate=pl.CostEstimate(flops=flops, bytes_accessed=moved, transcendentals=0),
    )(*inputs)


def shards(radiation, electrons, cell_index, cell_offset, kernel_x, kernel_y):
    cuts, dom = lax.axis_size("cuts"), lax.axis_size("dom")
    rows, slices, _ = radiation.shape
    half = kernel_x.shape[1]
    columns = kernel_y.shape[1]
    team = dom // slices
    groups = cuts * slices
    me = lax.axis_index("dom")
    mine = me // team
    cut = lax.axis_index("cuts")

    def seat(cut, number):
        return (1 - cut % 2) * number + (cut % 2) * (slices - 1 - number)

    def number(cut, team_number):
        return cut * slices + seat(cut, team_number)

    group = number(cut, mine)
    tiles = electrons.shape[2] // TILE

    def move(value, target):
        route = []
        for cut in range(cuts):
            for place in range(dom):
                to_cut, to_place = target(cut, place)
                route.append((cut * dom + place, to_cut * dom + to_place))
        return lax.ppermute(value, ("cuts", "dom"), route)

    def pick(array, which):
        return lax.dynamic_index_in_dim(array, which, 0, keepdims=False)

    def to_group(shift, turn=0):
        def target(cut, place):
            home = (number(cut, place // team) + shift) % groups
            return home // slices, seat(home // slices, (home + turn) % slices) * team + place % team

        return target

    def across(value):
        return move(value, lambda cut, place: (cut, place ^ 1))

    (payload,) = call(
        pack_kernel,
        [pltpu.with_memory_space_constraint(array, pltpu.HBM) for array in (radiation, electrons, cell_index, cell_offset)],
        [(slices, 2 * rows + 6 * tiles, columns)],
        [],
        0,
    )
    kx_parts, ky_parts = call(
        parts_kernel, [kernel_x, kernel_y], [jax.ShapeDtypeStruct((6,) + kernel_x.shape[1:], bf16)] * 2, [], 0
    )
    masks = range(0, dom, 2)
    own_blocks = []
    for mask in masks:
        block = pick(payload, seat(cut, (me ^ mask) // team))
        if mask:
            block = move(block, lambda cut, place: (cut, place ^ mask))
        own_blocks.append(block)
    other_blocks = []
    for block in own_blocks:
        other_blocks.append(across(block[: 2 * rows]))
    where = jnp.stack([me ^ mask for mask in masks] + [me ^ 1 ^ mask for mask in masks]).astype(jnp.int32)

    field_shape = (2 * half, columns)
    state_shape = (2, len(masks) * tiles, TILE)
    cells_shape = (6,) + state_shape[1:]
    pair = pltpu.VMEM(state_shape, f32)
    splits = [pltpu.VMEM(field_shape, bf16)] * 2 + [pair] * 2
    work = 4 * 2 * half * columns * state_shape[1] * TILE
    state, cells = call(lay_kernel, own_blocks, [state_shape, cells_shape], [], 0)
    cells_of = [cells]
    for _ in range(1, ITERS):
        cells_of.append(move(cells_of[-1], to_group(-1)))
    field, amp = call(
        first_kernel, [where, cells] + own_blocks + other_blocks, [field_shape, state_shape], splits, work
    )
    for step in range(ITERS):
        if step > 0:
            fresh = ((group + step) % groups == 0).astype(jnp.int32).reshape(1)
            field, amp = call(
                gather_kernel,
                [fresh, own, other, kx_parts, ky_parts, cells_of[step]],
                [field_shape, state_shape],
                splits,
                work,
            )
        own, state = call(
            push_kernel,
            [amp, state, cells_of[step], field],
            [field_shape, state_shape],
            [pltpu.VMEM((8,) + state_shape[1:], f32), pair],
            work,
        )
        other = across(own)
        if step < ITERS - 1:
            state = move(state, to_group(-1))

    def places(home):
        return [seat(home // slices, (home + turn) % slices) * team + me % team for turn in range(slices)]

    field_home = (group + ITERS) % groups
    (blocks,) = call(
        last_kernel,
        [jnp.stack(places(field_home)).astype(jnp.int32), own, other, kx_parts, ky_parts],
        [(slices, 2 * rows, columns)],
        [],
        work // 16,
    )
    blocks, state = lax.optimization_barrier((blocks, state))
    landed = []
    for turn in range(slices):
        landed.append(move(blocks[turn], to_group(ITERS, turn)))
    state_home = (group + ITERS - 1) % groups
    seats = places(state_home)
    returned = []
    for turn in range(slices):
        chunk = (seats[turn] ^ seats[0]) // 2
        block = lax.dynamic_slice_in_dim(state, chunk * tiles, tiles, 1)
        returned.append(move(block, to_group(ITERS - 1, turn)))
    order = jnp.stack([(seat(cut, mine) - n) % slices for n in range(slices)]).astype(jnp.int32)
    zero = jnp.stack([group - seat(cut, mine) + n == 0 for n in range(slices)]).astype(jnp.int32)
    return tuple(call(final_kernel, [order, zero] + landed + returned, [radiation.shape, electrons.shape], [], 0))


def solution(mesh):
    placed = (
        P("dom", "cuts", None),
        P(None, "cuts", "dom"),
        P(None, "cuts", "dom"),
        P(None, "cuts", "dom"),
        P(),
        P(),
    )

    return jax.shard_map(
        shards,
        mesh=mesh,
        in_specs=placed,
        out_specs=(P("dom", "cuts", None), P(None, "cuts", "dom")),
        check_vma=False,
    )
```
